32 devices in a mesh: groups: 2 (over x), rows: 16 (over z, y, core).
Axes of the slice: x: 2, y: 2, z: 4, core: 2. Of those that a mesh axis runs over, the one named last changes fastest.
Arguments:
- frames: bfloat16 [16384, 2560], P(('groups', 'rows')), parts along dimension 0, may hold values from -6 to 6
- offsets: int32 [4096], P(('groups', 'rows')), parts along dimension 0, may hold values from 0 to 8173, as said below
- neighbours: int32 [32, 4096], P(None, ('groups', 'rows')), parts along dimension 1, may hold values from 0 to 2047, as said below
- initial_codes: int32 [32, 4096], P(None, ('groups', 'rows')), parts along dimension 1, may hold values from -1048576 to 1048575
- embed_weight: bfloat16 [2560, 256], replicated, may hold values from -0.125 to 0.125
- embed_bias: float32 [256], replicated, may hold values from -0.9 to 0.9
Outputs:
- affinity: float32 [32, 4096], P(None, ('groups', 'rows')), parts along dimension 1
- vectors: float32 [32, 4096], P(None, ('groups', 'rows')), parts along dimension 1
The draws below stay inside these ranges and needn't reach their ends.
There are 2 independent parts, one for each index of `groups`. The reference program is written for one: setup_inputs(seed, part) draws one part's arguments, and reference() takes and returns one part's arrays. A program takes and returns all parts, laid end to end along the dimension named above; an argument that names none is the same for every part. Nothing has to cross between parts.
Inputs may be any that keep to these rules, and one draw needn't show every extreme that they name: `offsets`: the window of row i starts in the block of 512 frames numbered i // 128 and its 19 frames end before frame 8192. `neighbours`: the 32 columns of row i are distinct and differ from i; the k-th is (i + d) mod 2048 with 1 + k s <= d <= (k + 1) s, where s = 63.
All inputs are finite; a program needn't handle non-finite values.
Results may differ from the reference program's by a relative error of at most 0.012.
The reference program's roundings to bfloat16 on the way (of `pooled` and `unit_rows`) count: a program that leaves them out, or rounds other values in their place, can miss the bound.
Values may be sent and summed in bfloat16 or wider, within the bound.
A program may use at most 64 MiB of HBM per device.

```python
from functools import partial
import jax
import jax.numpy as jnp
from jax import lax

C = 2560
EMB = 256
WIN = 19
K = 32
V = 32
ITERS = 3
ROWS_DEV = 128
FR_DEV = 512
N = 2048
NFR = 8192


def draw_offsets(key, part):
    row_ids = jnp.arange(N, dtype=jnp.int32)
    device = row_ids // ROWS_DEV
    inside = row_ids % ROWS_DEV
    inner_key = jax.random.fold_in(key, 11)
    rim_key = jax.random.fold_in(key, 12)
    spread = jax.random.randint(inner_key, (N,), 0, FR_DEV - WIN + 1, dtype=jnp.int32)
    rim_pick = jax.random.randint(rim_key, (N,), 0, WIN - 1, dtype=jnp.int32)
    crossing = (inside == ROWS_DEV - 1) & (device < N // ROWS_DEV - 1)
    local_start = jnp.where(crossing, FR_DEV - 1 - rim_pick, spread)
    return device * FR_DEV + local_start


def draw_neighbours(key, part):
    stride = (N - 1) // K
    jitter = jax.random.randint(jax.random.fold_in(key, 21), (K, N), 0, stride, dtype=jnp.int32)
    band = jnp.arange(K, dtype=jnp.int32)[:, None] * stride
    row_ids = jnp.arange(N, dtype=jnp.int32)[None, :]
    return (row_ids + 1 + band + jitter) % N


def with_ends(entries, stream_key, least, largest):
    spot = [jax.random.randint(jax.random.fold_in(stream_key, axis), (), 0, length) for axis, length in enumerate(entries.shape)]
    main_axis = entries.shape.index(max(entries.shape))
    next_to = spot[:main_axis] + [(spot[main_axis] + 1) % entries.shape[main_axis]] + spot[main_axis + 1:]
    return entries.at[tuple(spot)].set(least).at[tuple(next_to)].set(largest)


def block_levels(stream_key, dims, shards, least, top_value):
    def one(position, parts):
        draws = jax.random.uniform(jax.random.fold_in(jax.random.fold_in(stream_key, 6), position), (parts,), jnp.float32, least / len(shards), top_value / len(shards))
        return jnp.repeat(jnp.exp(draws), dims[position] // parts).reshape((-1,) + (1,) * (len(dims) - position - 1))

    gain = one(*shards[0])
    for cut in shards[1:]:
        gain = gain * one(*cut)
    return gain


def gaussian(own_key, shape, deviation, limit, cuts=(), kind=jnp.bfloat16):
    drawn = deviation * jax.random.normal(own_key, shape, jnp.float32)
    if cuts:
        drawn = drawn * block_levels(own_key, shape, cuts, -0.22, 0.18)
    return jnp.clip(drawn, -limit, limit).astype(kind)


def setup_inputs(seed: int = 0, part: int = 0) -> dict:
    keys = jax.random.split(jax.random.key(seed), 7)
    own_keys = jax.random.split(jax.random.fold_in(keys[6], part), 7)
    frames = gaussian(own_keys[0], (NFR, C), 1.0, 6.0, ((0, 16),))
    offsets = draw_offsets(jax.random.fold_in(jax.random.fold_in(keys[6], part), 71), part)
    neighbours = draw_neighbours(jax.random.fold_in(jax.random.fold_in(keys[6], part), 71), part)
    initial_codes = with_ends(jax.random.randint(own_keys[3], (V, N), -1048576, 1048576), jax.random.fold_in(own_keys[3], 1), -1048576, 1048575).astype(jnp.int32)
    embed_weight = gaussian(keys[4], (C, EMB), C ** -0.5, 0.125)
    embed_bias = gaussian(keys[5], (EMB,), 0.15, 0.9, (), jnp.float32)
    return dict(frames=frames, offsets=offsets, neighbours=neighbours, initial_codes=initial_codes, embed_weight=embed_weight, embed_bias=embed_bias)


epsilon = 1e-06
sharpness = 8.0
seed_scale = 2.0 ** (-20)

def pool_block(frames, block_offsets):

    def one_window(anchor):
        return lax.dynamic_slice_in_dim(frames, anchor, WIN, 0)
    windows = jax.vmap(one_window)(block_offsets)
    return (lax.optimization_barrier(jnp.sum(windows.astype(jnp.float32), axis=1)) * (1.0 / WIN)).astype(jnp.bfloat16)

def reference(frames, offsets, neighbours, initial_codes, embed_weight, embed_bias):
    pooled = lax.map(partial(pool_block, frames), offsets.reshape(-1, ROWS_DEV)).reshape(N, C)
    embedded = jnp.dot(pooled.astype(jnp.float32), embed_weight.astype(jnp.float32), preferred_element_type=jnp.float32) + embed_bias
    squares = lax.optimization_barrier(jnp.sum(embedded * embedded, axis=1, keepdims=True))
    unit_rows = (embedded * lax.rsqrt(squares + epsilon)).astype(jnp.bfloat16)
    columns = neighbours.T.reshape(-1, ROWS_DEV, K)

    def cosine_block(packed):
        rows_block, cols_block = packed
        neighbour_rows = jnp.take(unit_rows, cols_block, axis=0)
        return jnp.einsum('be,bke->bk', rows_block.astype(jnp.float32), neighbour_rows.astype(jnp.float32), precision=lax.Precision.HIGHEST)
    cosine = lax.map(cosine_block, (unit_rows.reshape(-1, ROWS_DEV, EMB), columns)).reshape(N, K).T
    affinity = jnp.exp(sharpness * (cosine - 1.0))
    vectors = initial_codes.astype(jnp.float32) * seed_scale
    for turn_index in range(ITERS):
        forward = lax.optimization_barrier(jnp.sum(affinity[None] * jnp.take(vectors, neighbours, axis=1), axis=1))
        backward = jnp.zeros_like(vectors).at[:, neighbours.reshape(-1)].add((affinity[None] * vectors[:, None, :]).reshape(vectors.shape[0], -1))
        mixed = 0.5 * (forward + backward)
        gram_matrix = jnp.dot(mixed, mixed.T, precision=lax.Precision.HIGHEST)
        cholesky_factor = jnp.linalg.cholesky(gram_matrix)
        vectors = jax.scipy.linalg.solve_triangular(cholesky_factor, mixed, lower=True)
    return (affinity, vectors)
```

```python
import functools

import jax
import jax.numpy as jnp
from jax import lax
from jax.experimental import pallas as pl
from jax.experimental.pallas import tpu as pltpu
from jax.sharding import PartitionSpec as P

WIN = 19
ITERS = 3
HALO = 32

epsilon = 1e-06
sharpness = 8.0
seed_scale = 2.0 ** (-20)
HIGH = lax.Precision.HIGHEST


def bands(block, count, rows, kept):
    total = count * rows
    stride = (total - 1) // kept
    found = set()
    for delta in range(1 - rows, rows):
        distance = (rows * block + delta) % total
        if distance >= 1 and (distance - 1) // stride < kept:
            found.add((distance - 1) // stride)
    return sorted(found)


def split(value):
    high = value.astype(jnp.bfloat16)
    low = (value - high.astype(jnp.float32)).astype(jnp.bfloat16)
    return high, low


def inverse_factor(gram):
    size = gram.shape[0]
    row = lax.broadcasted_iota(jnp.int32, (size, size), 0)
    lane = lax.broadcasted_iota(jnp.int32, (size, size), 1)
    eye = jnp.where(row == lane, 1.0, 0.0).astype(jnp.float32)
    work = jnp.concatenate([gram, eye], axis=1)
    tall = lax.broadcasted_iota(jnp.int32, (size, 1), 0)
    for j in range(size):
        pivot_row = work[j : j + 1, :]
        factor = work[:, j : j + 1] * (1.0 / work[j : j + 1, j : j + 1])
        work = work - jnp.where(tall > j, factor, 0.0) * pivot_row
    diagonal = jnp.sum(jnp.where(row == lane, work[:, :size], 0.0), axis=1, keepdims=True)
    return work[:, size:] * lax.rsqrt(diagonal)


def kernel(
    n, frames, weight, offsets, neighbours, codes, bias, affinity, vectors,
    frames_v, weight_v, halo, sums, units, starts, masks, s_high, s_low, mixes, grams,
    load_sem, halo_sem, send_sem, recv_sem, hop_sem,
):
    own_frames, channels = frames.shape
    kept, rows = neighbours.shape
    vec = codes.shape[0]
    total = n * rows
    me = lax.axis_index("rows")
    odd = lax.rem(me, 2)
    sibling = me + 1 - 2 * odd
    shift = 2 * odd - 1
    chunk = 512 if channels % 512 == 0 else 128
    chunks = channels // chunk

    loads = []
    for c in range(chunks):
        cut = pl.ds(c * chunk, chunk)
        loads.append(pltpu.make_async_copy(frames.at[:, cut], frames_v.at[:, cut], load_sem.at[c]))
    weight_load = pltpu.make_async_copy(weight, weight_v, load_sem.at[chunks])
    for load in loads:
        load.start()
    weight_load.start()

    barrier = pltpu.get_barrier_semaphore()
    for ahead in range(1, n):
        pl.semaphore_signal(barrier, inc=1, device_id={"rows": lax.rem(me + ahead, n)})

    starts[0, :vec, :] = codes[...].astype(jnp.float32) * seed_scale
    first = me * rows
    relative = neighbours[...] - first
    relative = jnp.where(relative < 0, relative + total, relative).astype(jnp.float32)
    starts[0, vec:, :] = relative

    pl.semaphore_wait(barrier, n - 1)

    sent = []

    def remote(src, dst, a, b, target):
        return pltpu.make_async_remote_copy(
            src_ref=src, dst_ref=dst, send_sem=a, recv_sem=b, device_id={"rows": target}
        )

    def launch(buffer, phase):
        order = []
        for c in range(1, n // 4 + 1):
            order.append(2 * c)
            if n - 2 * c != 2 * c:
                order.append(n - 2 * c)
        order = sorted(set(e for e in order if 0 < e < n))
        order = sorted(order, key=lambda e: -min(e, n - e))
        near = remote(
            buffer.at[0], buffer.at[lax.rem(shift + n, n)], hop_sem.at[phase, 0],
            recv_sem.at[phase, lax.rem(shift + n, n)], sibling,
        )
        near.start()
        sent.append(near)
        for e in order:
            copy = remote(
                buffer.at[0], buffer.at[n - e], send_sem.at[phase, e],
                recv_sem.at[phase, n - e], lax.rem(me + e, n),
            )
            copy.start()
            sent.append(copy)

    def arrived(buffer, phase, r):
        remote(
            buffer.at[0], buffer.at[r], send_sem.at[phase, r], recv_sem.at[phase, r], sibling
        ).wait_recv()

    def forward_on(buffer, phase, e):
        slot = lax.rem(e + shift + n, n)
        copy = remote(
            buffer.at[e], buffer.at[slot], hop_sem.at[phase, e], recv_sem.at[phase, slot], sibling
        )
        copy.start()
        sent.append(copy)

    arrival_order = sorted(range(2, n, 2), key=lambda e: min(e, n - e))

    behind = lax.rem(me + n - 1, n)
    halo_copy = remote(
        frames.at[pl.ds(0, HALO), :], halo, halo_sem.at[0], halo_sem.at[1], behind
    )
    halo_copy.start()
    launch(starts, 0)

    begins = offsets[...] - me * own_frames
    begins = jnp.transpose(jnp.broadcast_to(begins, (rows, rows)))
    column = lax.broadcasted_iota(jnp.int32, (rows, rows), 1)

    def window(base, width):
        pieces = []
        for at in range(0, width, rows):
            size = min(rows, width - at)
            position = (column + (base + at))[:, :size]
            start = begins[:, :size]
            inside = (position >= start) & (position < start + WIN)
            pieces.append(jnp.where(inside, 1.0, 0.0).astype(jnp.bfloat16))
        return jnp.concatenate(pieces, axis=1) if len(pieces) > 1 else pieces[0]

    body_mask = window(0, own_frames)
    rim_mask = window(own_frames, HALO)
    for c in range(chunks):
        cut = pl.ds(c * chunk, chunk)
        loads[c].wait()
        sums[:, cut] = jnp.dot(body_mask, frames_v[:, cut], preferred_element_type=jnp.float32)
    weight_load.wait()
    halo_copy.wait_recv()
    embedded = jnp.zeros((rows, weight.shape[1]), jnp.float32)
    for c in range(chunks):
        cut = pl.ds(c * chunk, chunk)
        whole = sums[:, cut] + jnp.dot(rim_mask, halo[:, cut], preferred_element_type=jnp.float32)
        pooled = (whole * (1.0 / WIN)).astype(jnp.bfloat16)
        embedded = embedded + jnp.dot(pooled, weight_v[cut, :], preferred_element_type=jnp.float32)
    embedded = embedded + bias[...]
    squares = jnp.sum(embedded * embedded, axis=1, keepdims=True)
    units[0] = (embedded * lax.rsqrt(squares + epsilon)).astype(jnp.bfloat16)
    launch(units, 1)

    for e in arrival_order:
        arrived(starts, 0, e)
        forward_on(starts, 0, e)
    down = lax.broadcasted_iota(jnp.int32, (rows, rows), 0).astype(jnp.float32)
    for r in [0] + arrival_order + list(range(1, n, 2)):
        if r % 2 == 1:
            arrived(starts, 0, r)
        mine = jnp.zeros((rows, rows), jnp.float32)
        for k in bands(r, n, rows, kept):
            mine = jnp.where(down == starts[0, vec + k : vec + k + 1, :] - rows * r, 0.5, mine)
        back = (n - r) % n
        theirs = jnp.zeros((rows, rows), jnp.float32)
        for k in bands(back, n, rows, kept):
            theirs = jnp.where(down == starts[r, vec + k : vec + k + 1, :] - rows * back, 0.5, theirs)
        masks[r] = mine + jnp.transpose(theirs)

    affinity[...] = jnp.zeros_like(affinity)
    mine_units = units[0]

    def score(r):
        scores = lax.dot_general(
            units[r], mine_units, (((1,), (1,)), ((), ())), preferred_element_type=jnp.float32
        )
        dense = jnp.exp(sharpness * (scores - 1.0))
        high, low = split(dense * masks[r])
        s_high[pl.ds(r * rows, rows), :] = high
        s_low[pl.ds(r * rows, rows), :] = low
        for k in bands(r, n, rows, kept):
            hit = down == starts[0, vec + k : vec + k + 1, :] - rows * r
            affinity[k : k + 1, :] += jnp.sum(jnp.where(hit, dense, 0.0), axis=0, keepdims=True)

    score(0)
    for e in arrival_order:
        arrived(units, 1, e)
        forward_on(units, 1, e)
        score(e)
    for r in range(1, n, 2):
        arrived(units, 1, r)
        score(r)

    def product(wide):
        out = jnp.zeros((vec, rows), jnp.float32)
        step = min(total, 2048)
        for at in range(0, total, step):
            high, low = split(wide[:, at : at + step])
            cut = pl.ds(at, step)
            both = jnp.dot(
                jnp.concatenate([high, low], axis=0), s_high[cut, :],
                preferred_element_type=jnp.float32,
            )
            rest = jnp.dot(high, s_low[cut, :], preferred_element_type=jnp.float32)
            out = out + (both[:vec] + (both[vec:] + rest))
        return out

    def gram_of(wide):
        return lax.dot_general(
            wide, wide, (((1,), (1,)), ((), ())), precision=HIGH,
            preferred_element_type=jnp.float32,
        )

    mixed = product(jnp.concatenate([starts[r, :vec, :] for r in range(n)], axis=1))
    for turn in range(ITERS - 1):
        buffer, phase = mixes.at[turn], 2 + turn
        buffer[0] = mixed
        launch(buffer, phase)
        for e in arrival_order:
            arrived(buffer, phase, e)
            forward_on(buffer, phase, e)
        for r in range(1, n, 2):
            arrived(buffer, phase, r)
        wide = jnp.concatenate([buffer[r] for r in range(n)], axis=1)
        factor = inverse_factor(gram_of(wide))
        mixed = jnp.dot(factor, product(wide), precision=HIGH, preferred_element_type=jnp.float32)

    phase = ITERS + 1
    part = gram_of(mixed)
    pack = vec // 8
    packed = jnp.concatenate([part[8 * i : 8 * i + 8, :] for i in range(pack)], axis=1)
    grams[0] = packed
    for ahead in range(1, n):
        copy = remote(
            grams.at[0], grams.at[n - ahead], send_sem.at[phase, ahead],
            recv_sem.at[phase, n - ahead], lax.rem(me + ahead, n),
        )
        copy.start()
        sent.append(copy)
    for r in range(1, n):
        arrived(grams, phase, r)
        packed = packed + grams[r]
    gram = jnp.concatenate([packed[:, vec * i : vec * i + vec] for i in range(pack)], axis=0)
    factor = inverse_factor(gram)
    vectors[...] = jnp.dot(factor, mixed, precision=HIGH, preferred_element_type=jnp.float32)
    halo_copy.wait_send()
    for copy in sent:
        copy.wait_send()


def solution(mesh):
    n = mesh.shape["rows"]

    def on_device(frames, offsets, neighbours, initial_codes, embed_weight, embed_bias):
        own_frames, channels = frames.shape
        kept, rows = neighbours.shape
        vec = initial_codes.shape[0]
        width = embed_weight.shape[1]
        here = pl.BlockSpec(memory_space=pltpu.VMEM)
        there = pl.BlockSpec(memory_space=pl.ANY)
        phases = ITERS + 2
        return pl.pallas_call(
            functools.partial(kernel, n),
            out_shape=(
                jax.ShapeDtypeStruct((kept, rows), jnp.float32),
                jax.ShapeDtypeStruct((vec, rows), jnp.float32),
            ),
            in_specs=[there, there, here, here, here, here],
            out_specs=(here, here),
            scratch_shapes=[
                pltpu.VMEM((own_frames, channels), jnp.bfloat16),
                pltpu.VMEM((channels, width), jnp.bfloat16),
                pltpu.VMEM((HALO, channels), jnp.bfloat16),
                pltpu.VMEM((rows, channels), jnp.float32),
                pltpu.VMEM((n, rows, width), jnp.bfloat16),
                pltpu.VMEM((n, vec + kept, rows), jnp.float32),
                pltpu.VMEM((n, rows, rows), jnp.float32),
                pltpu.VMEM((n * rows, rows), jnp.bfloat16),
                pltpu.VMEM((n * rows, rows), jnp.bfloat16),
                pltpu.VMEM((ITERS - 1, n, vec, rows), jnp.float32),
                pltpu.VMEM((n, 8, vec * vec // 8), jnp.float32),
                pltpu.SemaphoreType.DMA((channels // 128 + 1,)),
                pltpu.SemaphoreType.DMA((2,)),
                pltpu.SemaphoreType.DMA((phases, n)),
                pltpu.SemaphoreType.DMA((phases, n)),
                pltpu.SemaphoreType.DMA((phases, n)),
            ],
            compiler_params=pltpu.CompilerParams(
                collective_id=0, has_side_effects=True, vmem_limit_bytes=60 * 1024 * 1024
            ),
        )(
            frames, embed_weight, offsets.reshape(1, rows), neighbours, initial_codes,
            embed_bias.reshape(1, width),
        )

    placed = (
        P(("groups", "rows"), None),
        P(("groups", "rows")),
        P(None, ("groups", "rows")),
        P(None, ("groups", "rows")),
        P(),
        P(),
    )
    return jax.shard_map(
        on_device,
        mesh=mesh,
        in_specs=placed,
        out_specs=(P(None, ("groups", "rows")), P(None, ("groups", "rows"))),
        check_vma=False,
    )
```

```python
import functools

import jax
import jax.numpy as jnp
from jax import lax
from jax.experimental import pallas as pl
from jax.experimental.pallas import tpu as pltpu
from jax.sharding import PartitionSpec as P

WIN = 19
ITERS = 3
HALO = 32

epsilon = 1e-06
sharpness = 8.0
seed_scale = 2.0 ** (-20)
HIGH = lax.Precision.HIGHEST


def bands(block, count, rows, kept):
    total = count * rows
    stride = (total - 1) // kept
    found = set()
    for delta in range(1 - rows, rows):
        distance = (rows * block + delta) % total
        if distance >= 1 and (distance - 1) // stride < kept:
            found.add((distance - 1) // stride)
    return sorted(found)


def split(value):
    high = value.astype(jnp.bfloat16)
    low = (value - high.astype(jnp.float32)).astype(jnp.bfloat16)
    return high, low


def inverse_factor(gram):
    size = gram.shape[0]
    row = lax.broadcasted_iota(jnp.int32, (size, size), 0)
    lane = lax.broadcasted_iota(jnp.int32, (size, size), 1)
    eye = jnp.where(row == lane, 1.0, 0.0).astype(jnp.float32)
    work = jnp.concatenate([gram, eye], axis=1)
    tall = lax.broadcasted_iota(jnp.int32, work.shape, 0)
    group = 4 if size % 4 == 0 else 1
    for j in range(0, size, group):
        cols = [jnp.broadcast_to(work[:, j + t : j + t + 1], work.shape) for t in range(group)]
        lines = [work[j + t : j + t + 1, :] for t in range(group)]
        for t in range(group):
            factor = cols[t] * (1.0 / cols[t][j + t : j + t + 1, :])
            factor = jnp.where(tall > j + t, factor, 0.0)
            work = work - factor * lines[t]
            for u in range(t + 1, group):
                lines[u] = lines[u] - factor[j + u : j + u + 1, :] * lines[t]
                cols[u] = cols[u] - factor * cols[t][j + u : j + u + 1, :]
    diagonal = jnp.sum(jnp.where(row == lane, work[:, :size], 0.0), axis=1, keepdims=True)
    return work[:, size:] * lax.rsqrt(diagonal)


def kernel(
    n, frames, weight, offsets, neighbours, codes, bias, affinity, vectors,
    frames_v, weight_v, halo, sums, units, starts, masks, s_high, s_low, mixes, grams,
    load_sem, halo_sem, send_sem, recv_sem, hop_sem,
):
    own_frames, channels = frames.shape
    kept, rows = neighbours.shape
    vec = codes.shape[0]
    total = n * rows
    me = lax.axis_index("rows")
    odd = lax.rem(me, 2)
    sibling = me + 1 - 2 * odd
    shift = 2 * odd - 1
    chunk = 512 if channels % 512 == 0 else 128
    chunks = channels // chunk

    loads = []
    for c in range(chunks):
        cut = pl.ds(c * chunk, chunk)
        loads.append(pltpu.make_async_copy(frames.at[:, cut], frames_v.at[:, cut], load_sem.at[c]))
    weight_load = pltpu.make_async_copy(weight, weight_v, load_sem.at[chunks])
    for load in loads:
        load.start()
    weight_load.start()

    barrier = pltpu.get_barrier_semaphore()
    for ahead in range(1, n):
        pl.semaphore_signal(barrier, inc=1, device_id={"rows": lax.rem(me + ahead, n)})

    starts[0, :vec, :] = codes[...].astype(jnp.float32) * seed_scale
    first = me * rows
    relative = neighbours[...] - first
    relative = jnp.where(relative < 0, relative + total, relative).astype(jnp.float32)
    starts[0, vec:, :] = relative

    pl.semaphore_wait(barrier, n - 1)

    sent = []

    def remote(src, dst, a, b, target):
        return pltpu.make_async_remote_copy(
            src_ref=src, dst_ref=dst, send_sem=a, recv_sem=b, device_id={"rows": target}
        )

    def launch(buffer, phase):
        order = []
        for c in range(1, n // 4 + 1):
            order.append(2 * c)
            if n - 2 * c != 2 * c:
                order.append(n - 2 * c)
        order = sorted(set(e for e in order if 0 < e < n))
        order = sorted(order, key=lambda e: -min(e, n - e))
        near = remote(
            buffer.at[0], buffer.at[lax.rem(shift + n, n)], hop_sem.at[phase, 0],
            recv_sem.at[phase, lax.rem(shift + n, n)], sibling,
        )
        near.start()
        sent.append(near)
        for e in order:
            copy = remote(
                buffer.at[0], buffer.at[n - e], send_sem.at[phase, e],
                recv_sem.at[phase, n - e], lax.rem(me + e, n),
            )
            copy.start()
            sent.append(copy)

    def arrived(buffer, phase, r):
        remote(
            buffer.at[0], buffer.at[r], send_sem.at[phase, r], recv_sem.at[phase, r], sibling
        ).wait_recv()

    def forward_on(buffer, phase, e):
        slot = lax.rem(e + shift + n, n)
        copy = remote(
            buffer.at[e], buffer.at[slot], hop_sem.at[phase, e], recv_sem.at[phase, slot], sibling
        )
        copy.start()
        sent.append(copy)

    arrival_order = sorted(range(2, n, 2), key=lambda e: min(e, n - e))

    behind = lax.rem(me + n - 1, n)
    halo_copy = remote(
        frames.at[pl.ds(0, HALO), :], halo, halo_sem.at[0], halo_sem.at[1], behind
    )
    halo_copy.start()
    launch(starts, 0)

    begins = offsets[...] - me * own_frames
    begins = jnp.transpose(jnp.broadcast_to(begins, (rows, rows)))
    column = lax.broadcasted_iota(jnp.int32, (rows, rows), 1)

    def window(base, width):
        pieces = []
        for at in range(0, width, rows):
            size = min(rows, width - at)
            position = (column + (base + at))[:, :size]
            start = begins[:, :size]
            inside = (position >= start) & (position < start + WIN)
            pieces.append(jnp.where(inside, 1.0, 0.0).astype(jnp.bfloat16))
        return jnp.concatenate(pieces, axis=1) if len(pieces) > 1 else pieces[0]

    body_mask = window(0, own_frames)
    rim_mask = window(own_frames, HALO)
    for c in range(chunks):
        cut = pl.ds(c * chunk, chunk)
        loads[c].wait()
        sums[:, cut] = jnp.dot(body_mask, frames_v[:, cut], preferred_element_type=jnp.float32)
    weight_load.wait()
    halo_copy.wait_recv()
    embedded = jnp.zeros((rows, weight.shape[1]), jnp.float32)
    for c in range(chunks):
        cut = pl.ds(c * chunk, chunk)
        whole = sums[:, cut] + jnp.dot(rim_mask, halo[:, cut], preferred_element_type=jnp.float32)
        pooled = (whole * (1.0 / WIN)).astype(jnp.bfloat16)
        embedded = embedded + jnp.dot(pooled, weight_v[cut, :], preferred_element_type=jnp.float32)
    embedded = embedded + bias[...]
    squares = jnp.sum(embedded * embedded, axis=1, keepdims=True)
    units[0] = (embedded * lax.rsqrt(squares + epsilon)).astype(jnp.bfloat16)
    launch(units, 1)

    for e in arrival_order:
        arrived(starts, 0, e)
        forward_on(starts, 0, e)
    down = lax.broadcasted_iota(jnp.int32, (rows, rows), 0).astype(jnp.float32)
    for r in [0] + arrival_order + list(range(1, n, 2)):
        if r % 2 == 1:
            arrived(starts, 0, r)
        mine = jnp.zeros((rows, rows), jnp.float32)
        for k in bands(r, n, rows, kept):
            mine = jnp.where(down == starts[0, vec + k : vec + k + 1, :] - rows * r, 0.5, mine)
        back = (n - r) % n
        theirs = jnp.zeros((rows, rows), jnp.float32)
        for k in bands(back, n, rows, kept):
            theirs = jnp.where(down == starts[r, vec + k : vec + k + 1, :] - rows * back, 0.5, theirs)
        masks[r] = mine + jnp.transpose(theirs)

    affinity[...] = jnp.zeros_like(affinity)
    mine_units = units[0]

    def score(r):
        scores = lax.dot_general(
            units[r], mine_units, (((1,), (1,)), ((), ())), preferred_element_type=jnp.float32
        )
        dense = jnp.exp(sharpness * (scores - 1.0))
        high, low = split(dense * masks[r])
        s_high[pl.ds(r * rows, rows), :] = high
        s_low[pl.ds(r * rows, rows), :] = low
        for k in bands(r, n, rows, kept):
            hit = down == starts[0, vec + k : vec + k + 1, :] - rows * r
            affinity[k : k + 1, :] += jnp.sum(jnp.where(hit, dense, 0.0), axis=0, keepdims=True)

    score(0)
    for e in arrival_order:
        arrived(units, 1, e)
        forward_on(units, 1, e)
        score(e)
    for r in range(1, n, 2):
        arrived(units, 1, r)
        score(r)

    def product(wide):
        out = jnp.zeros((vec, rows), jnp.float32)
        step = min(total, 2048)
        for at in range(0, total, step):
            high, low = split(wide[:, at : at + step])
            cut = pl.ds(at, step)
            both = jnp.dot(
                jnp.concatenate([high, low], axis=0), s_high[cut, :],
                preferred_element_type=jnp.float32,
            )
            rest = jnp.dot(high, s_low[cut, :], preferred_element_type=jnp.float32)
            out = out + (both[:vec] + (both[vec:] + rest))
        return out

    def gram_of(wide):
        return lax.dot_general(
            wide, wide, (((1,), (1,)), ((), ())), precision=HIGH,
            preferred_element_type=jnp.float32,
        )

    def apply(factor, value):
        return jnp.dot(factor, value, precision=HIGH, preferred_element_type=jnp.float32)

    mixed = product(jnp.concatenate([starts[r, :vec, :] for r in range(n)], axis=1))
    pending = None
    for turn in range(ITERS - 1):
        buffer, phase = mixes.at[turn], 2 + turn
        buffer[0] = mixed
        launch(buffer, phase)
        factor = None if pending is None else inverse_factor(gram_of(pending))
        for e in arrival_order:
            arrived(buffer, phase, e)
            forward_on(buffer, phase, e)
        for r in range(1, n, 2):
            arrived(buffer, phase, r)
        pending = jnp.concatenate([buffer[r] for r in range(n)], axis=1)
        if factor is not None:
            pending = apply(factor, pending)
        mixed = product(pending)
    mixed = apply(inverse_factor(gram_of(pending)), mixed)

    phase = ITERS + 1
    part = gram_of(mixed)
    pack = vec // 8
    packed = jnp.concatenate([part[8 * i : 8 * i + 8, :] for i in range(pack)], axis=1)
    grams[0] = packed
    for ahead in range(1, n):
        copy = remote(
            grams.at[0], grams.at[n - ahead], send_sem.at[phase, ahead],
            recv_sem.at[phase, n - ahead], lax.rem(me + ahead, n),
        )
        copy.start()
        sent.append(copy)
    for r in range(1, n):
        arrived(grams, phase, r)
        packed = packed + grams[r]
    gram = jnp.concatenate([packed[:, vec * i : vec * i + vec] for i in range(pack)], axis=0)
    factor = inverse_factor(gram)
    vectors[...] = apply(factor, mixed)
    halo_copy.wait_send()
    for copy in sent:
        copy.wait_send()


def solution(mesh):
    n = mesh.shape["rows"]

    def on_device(frames, offsets, neighbours, initial_codes, embed_weight, embed_bias):
        own_frames, channels = frames.shape
        kept, rows = neighbours.shape
        vec = initial_codes.shape[0]
        width = embed_weight.shape[1]
        here = pl.BlockSpec(memory_space=pltpu.VMEM)
        there = pl.BlockSpec(memory_space=pl.ANY)
        phases = ITERS + 2
        return pl.pallas_call(
            functools.partial(kernel, n),
            out_shape=(
                jax.ShapeDtypeStruct((kept, rows), jnp.float32),
                jax.ShapeDtypeStruct((vec, rows), jnp.float32),
            ),
            in_specs=[there, there, here, here, here, here],
            out_specs=(here, here),
            scratch_shapes=[
                pltpu.VMEM((own_frames, channels), jnp.bfloat16),
                pltpu.VMEM((channels, width), jnp.bfloat16),
                pltpu.VMEM((HALO, channels), jnp.bfloat16),
                pltpu.VMEM((rows, channels), jnp.float32),
                pltpu.VMEM((n, rows, width), jnp.bfloat16),
                pltpu.VMEM((n, vec + kept, rows), jnp.float32),
                pltpu.VMEM((n, rows, rows), jnp.float32),
                pltpu.VMEM((n * rows, rows), jnp.bfloat16),
                pltpu.VMEM((n * rows, rows), jnp.bfloat16),
                pltpu.VMEM((ITERS - 1, n, vec, rows), jnp.float32),
                pltpu.VMEM((n, 8, vec * vec // 8), jnp.float32),
                pltpu.SemaphoreType.DMA((channels // 128 + 1,)),
                pltpu.SemaphoreType.DMA((2,)),
                pltpu.SemaphoreType.DMA((phases, n)),
                pltpu.SemaphoreType.DMA((phases, n)),
                pltpu.SemaphoreType.DMA((phases, n)),
            ],
            compiler_params=pltpu.CompilerParams(
                collective_id=0, has_side_effects=True, vmem_limit_bytes=60 * 1024 * 1024
            ),
        )(
            frames, embed_weight, offsets.reshape(1, rows), neighbours, initial_codes,
            embed_bias.reshape(1, width),
        )

    placed = (
        P(("groups", "rows"), None),
        P(("groups", "rows")),
        P(None, ("groups", "rows")),
        P(None, ("groups", "rows")),
        P(),
        P(),
    )
    return jax.shard_map(
        on_device,
        mesh=mesh,
        in_specs=placed,
        out_specs=(P(None, ("groups", "rows")), P(None, ("groups", "rows"))),
        check_vma=False,
    )
```
